128 devices in a mesh: batch: 1, graph: 128 (over z, y, x, core).
Axes of the slice: x: 4, y: 4, z: 4, core: 2. Of those that a mesh axis runs over, the one named last changes fastest.
Arguments:
- grid_feat: float32 [65536, 102], P(('batch', 'graph'))
- mesh_feat: float32 [65536, 3], P(('batch', 'graph'))
- edge_feat: float32 [1048576, 4], P(('batch', 'graph'))
- need_rows: int32 [1048576], P(('batch', 'graph'))
- edge_src: int32 [1048576], P(('batch', 'graph'))
- edge_dst: int32 [1048576], P(('batch', 'graph'))
- edge_mask: int32 [1048576], P(('batch', 'graph'))
- w_grid_emb: bfloat16 [102, 1024], replicated
- w_mesh_emb: bfloat16 [3, 1024], replicated
- w_edge_emb: bfloat16 [4, 1024], replicated
- w_edge_upd: bfloat16 [3072, 1024], replicated
- w_mesh_upd: bfloat16 [2048, 1024], replicated
- w_grid_upd: bfloat16 [1024, 1024], replicated
- w_second: bfloat16 [6, 1024, 1024], replicated
- mlp_vecs: bfloat16 [6, 4, 1024], replicated
Outputs:
- output 1: bfloat16 [65536, 1024], P(('batch', 'graph'))
- output 2: bfloat16 [65536, 1024], P(('batch', 'graph'))
All inputs are finite; a program needn't handle non-finite values.
Results may differ from the reference program's by a relative error of at most 0.00922038.
Values are sent between devices in bfloat16 or wider.
A program may use at most 1 GiB of HBM per device.

```python
import jax
import jax.numpy as jnp
from jax import lax

GRAPH = 128
GRID_DEV = 512
MESH_DEV = 512
EDGE_DEV = 8192
TABLE_DEV = 8192
WIDTH = 1024
GRID_FEAT = 102
MESH_FEAT = 3
EDGE_FEAT = 4

SLOTS = TABLE_DEV // GRAPH
N_GRID = GRAPH * GRID_DEV
N_MESH = GRAPH * MESH_DEV
N_EDGE = GRAPH * EDGE_DEV
LN_EPS = 1e-5


def draw_graph(graph_key):
    keys = jax.random.split(graph_key, 8)
    stride = GRID_DEV // SLOTS
    spread_rows = (jnp.arange(SLOTS, dtype=jnp.int32) * stride)[None, None, :] + jax.random.randint(keys[0], (GRAPH, GRAPH, SLOTS), 0, stride, dtype=jnp.int32)
    row_shift = jax.random.randint(keys[7], (GRAPH, GRAPH, 1), 0, GRID_DEV, dtype=jnp.int32)
    need_rows = (spread_rows + row_shift) % GRID_DEV
    used = jax.random.randint(keys[1], (GRAPH, GRAPH), max(1, SLOTS // 4), SLOTS + 1, dtype=jnp.int32)
    owner = jax.random.randint(keys[2], (GRAPH, EDGE_DEV), 0, GRAPH, dtype=jnp.int32)
    slot = jax.random.randint(keys[3], (GRAPH, EDGE_DEV), 0, jnp.take_along_axis(used, owner, axis=1), dtype=jnp.int32)
    edge_dst = jax.random.randint(keys[4], (GRAPH, EDGE_DEV), 0, MESH_DEV, dtype=jnp.int32)
    keep_level = jax.random.randint(keys[5], (GRAPH, 1), 1, 5, dtype=jnp.int32)
    edge_mask = (jax.random.randint(keys[6], (GRAPH, EDGE_DEV), 0, 4, dtype=jnp.int32) < keep_level).astype(jnp.int32)
    edge_src = owner * SLOTS + slot
    return need_rows.reshape(-1), edge_src.reshape(-1), edge_dst.reshape(-1), edge_mask.reshape(-1)


def weight(key, fan_in, shape):
    return (jax.random.normal(key, shape, jnp.float32) * fan_in ** -0.5).astype(jnp.bfloat16)


def setup_inputs(seed: int = 0, part: int = 0) -> dict:
    part_key = jax.random.fold_in(jax.random.key(seed), part)
    part_keys = jax.random.split(part_key, 6)
    shared_keys = jax.random.split(jax.random.key(seed + 1), 8)
    lat_pos = (jnp.arange(N_GRID, dtype=jnp.float32) + 0.5) / N_GRID
    lat_freq = jax.random.randint(part_keys[0], (GRID_FEAT,), 1, 5, dtype=jnp.int32).astype(jnp.float32)
    phases = jax.random.uniform(part_keys[1], (GRID_FEAT,), jnp.float32, 0.0, 6.283)
    lat_wave = jnp.cos(jnp.pi * lat_pos[:, None] * lat_freq[None, :] + phases[None, :])
    grid_feat = jax.random.normal(part_keys[2], (N_GRID, GRID_FEAT), jnp.float32) + 1.5 * lat_wave
    mesh_feat = jax.random.normal(part_keys[3], (N_MESH, MESH_FEAT), jnp.float32)
    edge_feat = jax.random.normal(part_keys[4], (N_EDGE, EDGE_FEAT), jnp.float32)
    need_rows, edge_src, edge_dst, edge_mask = draw_graph(part_keys[5])
    vec_scale = jnp.array([0.5, 0.5, 0.3, 0.3], jnp.float32)[None, :, None]
    vec_shift = jnp.array([0.0, 0.0, 1.0, 0.0], jnp.float32)[None, :, None]
    mlp_vecs = (jax.random.normal(shared_keys[7], (6, 4, WIDTH), jnp.float32) * vec_scale + vec_shift).astype(jnp.bfloat16)
    return dict(grid_feat=grid_feat, mesh_feat=mesh_feat, edge_feat=edge_feat, need_rows=need_rows,
                edge_src=edge_src, edge_dst=edge_dst, edge_mask=edge_mask,
                w_grid_emb=weight(shared_keys[0], GRID_FEAT, (GRID_FEAT, WIDTH)),
                w_mesh_emb=weight(shared_keys[1], MESH_FEAT, (MESH_FEAT, WIDTH)),
                w_edge_emb=weight(shared_keys[2], EDGE_FEAT, (EDGE_FEAT, WIDTH)),
                w_edge_upd=weight(shared_keys[3], 3 * WIDTH, (3 * WIDTH, WIDTH)),
                w_mesh_upd=weight(shared_keys[4], 2 * WIDTH, (2 * WIDTH, WIDTH)),
                w_grid_upd=weight(shared_keys[5], WIDTH, (WIDTH, WIDTH)),
                w_second=weight(shared_keys[6], WIDTH, (6, WIDTH, WIDTH)),
                mlp_vecs=mlp_vecs)


def mlp_tail(pre_act, w_out, params):
    hidden = jax.nn.silu(pre_act + params[0].astype(jnp.float32)).astype(jnp.bfloat16)
    result = jnp.dot(hidden, w_out, preferred_element_type=jnp.float32) + params[1].astype(jnp.float32)
    mean = jnp.mean(result, axis=-1, keepdims=True)
    centered = result - mean
    variance = jnp.mean(centered * centered, axis=-1, keepdims=True)
    return centered * lax.rsqrt(variance + LN_EPS) * params[2].astype(jnp.float32) + params[3].astype(jnp.float32)


def mlp(features, w_in, w_out, params):
    pre_act = jnp.dot(features.astype(jnp.bfloat16), w_in, preferred_element_type=jnp.float32)
    return mlp_tail(pre_act, w_out, params)


def reference(grid_feat, mesh_feat, edge_feat, need_rows, edge_src, edge_dst, edge_mask,
              w_grid_emb, w_mesh_emb, w_edge_emb, w_edge_upd, w_mesh_upd, w_grid_upd, w_second, mlp_vecs):
    def grid_band(band_feat):
        grid_emb = mlp(band_feat, w_grid_emb, w_second[0], mlp_vecs[0]).astype(jnp.bfloat16)
        grid_new = (grid_emb.astype(jnp.float32) + mlp(grid_emb, w_grid_upd, w_second[5], mlp_vecs[5])).astype(jnp.bfloat16)
        return grid_emb, grid_new

    grid_emb, grid_out = lax.map(grid_band, grid_feat.reshape(GRAPH, GRID_DEV, GRID_FEAT))
    band_index = jnp.arange(GRAPH)[:, None]

    def mesh_shard(shard):
        mesh_dev, edge_dev, need_dev, src_dev, dst_dev, mask_dev = shard
        table = grid_emb[band_index, need_dev.reshape(GRAPH, SLOTS)].reshape(TABLE_DEV, WIDTH)
        mesh_emb = mlp(mesh_dev, w_mesh_emb, w_second[1], mlp_vecs[1]).astype(jnp.bfloat16)
        edge_emb = mlp(edge_dev, w_edge_emb, w_second[2], mlp_vecs[2]).astype(jnp.bfloat16)
        joined = jnp.concatenate([edge_emb, table[src_dev], mesh_emb[dst_dev]], axis=1)
        edge_new = (edge_emb.astype(jnp.float32) + mlp(joined, w_edge_upd, w_second[3], mlp_vecs[3])).astype(jnp.bfloat16)
        masked = edge_new.astype(jnp.float32) * mask_dev[:, None].astype(jnp.float32)
        aggregated = jax.ops.segment_sum(masked, dst_dev, num_segments=MESH_DEV).astype(jnp.bfloat16)
        mesh_in = jnp.concatenate([mesh_emb, aggregated], axis=1)
        return (mesh_emb.astype(jnp.float32) + mlp(mesh_in, w_mesh_upd, w_second[4], mlp_vecs[4])).astype(jnp.bfloat16)

    mesh_out = lax.map(mesh_shard, (mesh_feat.reshape(GRAPH, MESH_DEV, MESH_FEAT),
                                    edge_feat.reshape(GRAPH, EDGE_DEV, EDGE_FEAT),
                                    need_rows.reshape(GRAPH, TABLE_DEV),
                                    edge_src.reshape(GRAPH, EDGE_DEV),
                                    edge_dst.reshape(GRAPH, EDGE_DEV),
                                    edge_mask.reshape(GRAPH, EDGE_DEV)))
    return (mesh_out.reshape(N_MESH, WIDTH), grid_out.reshape(N_GRID, WIDTH))
```

```python
import functools

import jax
import jax.numpy as jnp
from jax import lax
from jax.experimental import pallas as pl
from jax.experimental.pallas import tpu as pltpu
from jax.sharding import PartitionSpec as P

LN_EPS = 1e-5
BF = jnp.bfloat16
F32 = jnp.float32
D = 1024
NODES = 512
EDGES = 8192
LANES = 128
SUB = 256
NC = 256
LN_ROWS = 32
ROWS1 = 1024
ROWS2 = 512
CHUNK = 4096


def silu(x):
    h = 0.5 * x
    return h + h * jnp.tanh(h)


def vec(vecs, mlp, k):
    return vecs[4 * mlp + k:4 * mlp + k + 1, :]


def layer_norm(x, gain, shift):
    mean = jnp.sum(x, axis=-1, keepdims=True) * (1.0 / D)
    c = x - mean
    var = jnp.sum(c * c, axis=-1, keepdims=True) * (1.0 / D)
    return c * lax.rsqrt(var + LN_EPS) * gain + shift


def first_layer(x, w, h, r0, bias=None):
    for n in range(D // NC):
        cols = slice(n * NC, (n + 1) * NC)
        pre = jnp.dot(x, w[:, cols], preferred_element_type=F32)
        if bias is not None:
            pre = pre + bias[:, cols]
        h[r0:r0 + SUB, cols] = silu(pre).astype(BF)


def second_layer(h, w, r, r0, bias):
    for n in range(D // NC):
        cols = slice(n * NC, (n + 1) * NC)
        r[r0:r0 + SUB, cols] = jnp.dot(h[r0:r0 + SUB, :], w[:, cols], preferred_element_type=F32) + bias[:, cols]


def norm_rows(r, r0, gain, shift, store):
    for q in range(0, SUB, LN_ROWS):
        store(r0 + q, layer_norm(r[r0 + q:r0 + q + LN_ROWS, :], gain, shift))


def embed_kernel(xe, a2, xg, a0, xm, a1, vecs, wsec, wedge, wgrid,
                 he_out, grid_out, hm_out, proj_out,
                 h, r, emb, wa, wb, wc, wd, we, wf, sems):
    i = pl.program_id(0)
    edge_steps = EDGES // ROWS1
    copies = [pltpu.make_async_copy(wsec.at[2], wa, sems.at[0]),
              pltpu.make_async_copy(wsec.at[0], wb, sems.at[1]),
              pltpu.make_async_copy(wgrid, wc, sems.at[2]),
              pltpu.make_async_copy(wsec.at[5], wd, sems.at[3]),
              pltpu.make_async_copy(wsec.at[1], we, sems.at[4]),
              pltpu.make_async_copy(wedge.at[pl.ds(2 * D, D)], wf, sems.at[5])]

    @pl.when(i == 0)
    def _():
        for c in copies:
            c.start()
        copies[0].wait()

    @pl.when(i < edge_steps)
    def _():
        blocks = range(0, ROWS1, SUB)
        for r0 in blocks:
            first_layer(xe[r0:r0 + SUB, :], a2, h, r0)
        for r0 in blocks:
            second_layer(h, wa, r, r0, vec(vecs, 2, 1))

            def store(row, y):
                he_out[row:row + LN_ROWS, :] = y.astype(BF)
            norm_rows(r, r0, vec(vecs, 2, 2), vec(vecs, 2, 3), store)

    blocks = range(0, NODES, SUB)

    @pl.when(i == edge_steps)
    def _():
        copies[1].wait()
        copies[2].wait()
        copies[3].wait()
        for r0 in blocks:
            first_layer(xg[r0:r0 + SUB, :], a0, h, r0)
        for r0 in blocks:
            second_layer(h, wb, r, r0, vec(vecs, 0, 1))

            def store(row, y):
                emb[row:row + LN_ROWS, :] = y.astype(BF)
            norm_rows(r, r0, vec(vecs, 0, 2), vec(vecs, 0, 3), store)
        for r0 in blocks:
            first_layer(emb[r0:r0 + SUB, :], wc, h, r0, vec(vecs, 5, 0))
        for r0 in blocks:
            second_layer(h, wd, r, r0, vec(vecs, 5, 1))

            def store_out(row, y):
                base = emb[row:row + LN_ROWS, :].astype(F32)
                grid_out[row:row + LN_ROWS, :] = (base + y).astype(BF)
            norm_rows(r, r0, vec(vecs, 5, 2), vec(vecs, 5, 3), store_out)

    @pl.when(i == edge_steps + 1)
    def _():
        copies[4].wait()
        copies[5].wait()
        for r0 in blocks:
            first_layer(xm[r0:r0 + SUB, :], a1, h, r0)
        for r0 in blocks:
            second_layer(h, we, r, r0, vec(vecs, 1, 1))

            def store(row, y):
                hm_out[row:row + LN_ROWS, :] = y.astype(BF)
            norm_rows(r, r0, vec(vecs, 1, 2), vec(vecs, 1, 3), store)
        for r0 in blocks:
            for n in range(D // NC):
                cols = slice(n * NC, (n + 1) * NC)
                p = jnp.dot(hm_out[r0:r0 + SUB, :], wf[:, cols], preferred_element_type=F32) + vec(vecs, 3, 0)[:, cols]
                for t in range(NC // LANES):
                    j = n * (NC // LANES) + t
                    proj_out[pl.ds(r0 * 8 + j, SUB, stride=8), :] = p[:, t * LANES:(t + 1) * LANES]


def edge_kernel(src_s, dst_s, need_s, he, dst_v, mask_v, a0, vecs, proj, hm, table, wsec, wedge, wmesh,
                mesh_out,
                ftab, stage, xg, gm, cat, h, r, new, acc, w0, w3, w12, sems):
    i = pl.program_id(0)
    steps = EDGES // ROWS2
    copies = [pltpu.make_async_copy(wsec.at[0], w0, sems.at[2]),
              pltpu.make_async_copy(wedge.at[pl.ds(0, 2 * D)], w12, sems.at[3]),
              pltpu.make_async_copy(wsec.at[3], w3, sems.at[4])]
    nchunk = table.shape[0] // CHUNK

    def stage_copy(c, slot):
        return pltpu.make_async_copy(table.at[pl.ds(pl.multiple_of(c * CHUNK, CHUNK), CHUNK)], stage.at[slot], sems.at[slot])

    def fetch_row(edge, row):
        s = src_s[edge]
        g = lax.shift_right_logical(s, 6) * 512 + need_s[s]
        xg[pl.ds(row, 1), :] = ftab[pl.ds(g, 1), :]

    @pl.when(i == 0)
    def _():
        stage_copy(0, 0).start()
        stage_copy(1, 1).start()
        for c in copies:
            c.start()

        def chunk(c, carry):
            slot = lax.rem(c, 2)
            stage_copy(c, slot).wait()

            def part(k, inner):
                rows = pl.multiple_of(k * 256, 256)
                ftab[pl.ds(pl.multiple_of(c * CHUNK + rows, 256), 256), :] = stage[slot, pl.ds(rows, 256), :].astype(F32)
                return inner
            lax.fori_loop(0, CHUNK // 256, part, 0)

            @pl.when(c + 2 < nchunk)
            def _():
                stage_copy(c + 2, slot).start()
            return carry
        lax.fori_loop(0, nchunk, chunk, 0)
        acc[...] = jnp.zeros_like(acc)

        def fetch8(k, carry):
            for t in range(8):
                fetch_row(k * 8 + t, k * 8 + t)
            return carry
        lax.fori_loop(0, ROWS2 // 8, fetch8, 0)
        for c in copies:
            c.wait()

    blocks = range(0, ROWS2, SUB)
    for r0 in blocks:
        first_layer(xg[r0:r0 + SUB, :].astype(BF), a0, h, r0)
    base = i * ROWS2
    after = jnp.minimum(i + 1, steps - 1) * ROWS2
    for e in range(ROWS2):
        d = dst_s[base + e]
        gm[e * 8:(e + 1) * 8, :] = proj[pl.ds(pl.multiple_of(d * 8, 8), 8), :]
        fetch_row(after + e, e)
    for r0 in blocks:
        cat[r0:r0 + SUB, :D] = he[r0:r0 + SUB, :]
        second_layer(h, w0, r, r0, vec(vecs, 0, 1))

        def store(row, y):
            cat[row:row + LN_ROWS, D:] = y.astype(BF)
        norm_rows(r, r0, vec(vecs, 0, 2), vec(vecs, 0, 3), store)
    for r0 in blocks:
        for n in range(D // NC):
            cols = slice(n * NC, (n + 1) * NC)
            pre = jnp.dot(cat[r0:r0 + SUB, :], w12[:, cols], preferred_element_type=F32)
            for t in range(NC // LANES):
                j = n * (NC // LANES) + t
                part = pre[:, t * LANES:(t + 1) * LANES] + gm[pl.ds(r0 * 8 + j, SUB, stride=8), :]
                h[r0:r0 + SUB, j * LANES:(j + 1) * LANES] = silu(part).astype(BF)
    for r0 in blocks:
        second_layer(h, w3, r, r0, vec(vecs, 3, 1))

        def store_new(row, y):
            new[row:row + LN_ROWS, :] = (he[row:row + LN_ROWS, :].astype(F32) + y).astype(BF)
        norm_rows(r, r0, vec(vecs, 3, 2), vec(vecs, 3, 3), store_new)
    for r0 in blocks:
        node = lax.broadcasted_iota(jnp.int32, (NODES, SUB), 0)
        dst = jnp.where(mask_v[0, :, r0:r0 + SUB] > 0, dst_v[0, :, r0:r0 + SUB], -1)
        inc = jnp.where(node == dst, 1.0, 0.0).astype(BF)
        for n in range(D // NC):
            cols = slice(n * NC, (n + 1) * NC)
            acc[:, cols] += jnp.dot(inc, new[r0:r0 + SUB, cols], preferred_element_type=F32)

    @pl.when(i == steps - 1)
    def _():
        last = [pltpu.make_async_copy(wmesh, w12, sems.at[3]),
                pltpu.make_async_copy(wsec.at[4], w0, sems.at[2])]
        for c in last:
            c.start()
        cat[:, :D] = hm[...]
        cat[:, D:] = acc[...].astype(BF)
        last[0].wait()
        for r0 in range(0, NODES, SUB):
            first_layer(cat[r0:r0 + SUB, :], w12, h, r0, vec(vecs, 4, 0))
        last[1].wait()
        for r0 in range(0, NODES, SUB):
            second_layer(h, w0, r, r0, vec(vecs, 4, 1))

            def store(row, y):
                mesh_out[row:row + LN_ROWS, :] = (hm[row:row + LN_ROWS, :].astype(F32) + y).astype(BF)
            norm_rows(r, r0, vec(vecs, 4, 2), vec(vecs, 4, 3), store)


def fixed(shape):
    return pl.BlockSpec(shape, lambda i, *_: (0,) * len(shape), pipeline_mode=pl.Buffered(1))


ANY = pl.BlockSpec(memory_space=pl.ANY)


def run_embed(xe, a2, xg, a0, xm, a1, vecs, w_second, w_edge_upd, w_grid_upd):
    steps = EDGES // ROWS1
    flops = 2 * D * (EDGES * (D + LANES) + NODES * (5 * D + 2 * LANES))
    wvm = pltpu.VMEM((D, D), BF)
    return pl.pallas_call(
        embed_kernel,
        grid=(steps + 2,),
        in_specs=[pl.BlockSpec((ROWS1, LANES), lambda i: (jnp.minimum(i, steps - 1), 0)), fixed((LANES, D)),
                  fixed((NODES, LANES)), fixed((LANES, D)), fixed((NODES, LANES)), fixed((LANES, D)),
                  fixed((24, D)), ANY, ANY, ANY],
        out_specs=[pl.BlockSpec((ROWS1, D), lambda i: (jnp.minimum(i, steps - 1), 0)),
                   fixed((NODES, D)), fixed((NODES, D)), fixed((NODES * 8, LANES))],
        out_shape=[jax.ShapeDtypeStruct((EDGES, D), BF), jax.ShapeDtypeStruct((NODES, D), BF),
                   jax.ShapeDtypeStruct((NODES, D), BF), jax.ShapeDtypeStruct((NODES * 8, LANES), F32)],
        scratch_shapes=[pltpu.VMEM((ROWS1, D), BF), pltpu.VMEM((ROWS1, D), F32), pltpu.VMEM((NODES, D), BF),
                        wvm, wvm, wvm, wvm, wvm, wvm, pltpu.SemaphoreType.DMA((6,))],
        compiler_params=pltpu.CompilerParams(vmem_limit_bytes=56 << 20, dimension_semantics=("arbitrary",)),
        cost_estimate=pl.CostEstimate(flops=flops, bytes_accessed=36 << 20, transcendentals=0),
        name="embed",
    )(xe, a2, xg, a0, xm, a1, vecs, w_second, w_edge_upd, w_grid_upd)


def run_edges(src, dst, need, he, mask, a0, vecs, proj, hm, table, w_second, w_edge_upd, w_mesh_upd):
    steps = EDGES // ROWS2
    flops = 2 * D * (EDGES * (4 * D + LANES + NODES) + NODES * 3 * D)
    lanes = lambda i, *_: (i, 0, 0)
    grid_spec = pltpu.PrefetchScalarGridSpec(
        num_scalar_prefetch=3,
        grid=(steps,),
        in_specs=[pl.BlockSpec((ROWS2, D), lambda i, *_: (i, 0)),
                  pl.BlockSpec((1, 1, ROWS2), lanes), pl.BlockSpec((1, 1, ROWS2), lanes),
                  fixed((LANES, D)), fixed((24, D)), fixed((NODES * 8, LANES)), fixed((NODES, D)),
                  ANY, ANY, ANY, ANY],
        out_specs=fixed((NODES, D)),
        scratch_shapes=[pltpu.VMEM(table.shape, F32), pltpu.VMEM((2, CHUNK, LANES), BF),
                        pltpu.VMEM((ROWS2, LANES), F32), pltpu.VMEM((ROWS2 * 8, LANES), F32),
                        pltpu.VMEM((ROWS2, 2 * D), BF), pltpu.VMEM((ROWS2, D), BF), pltpu.VMEM((ROWS2, D), F32),
                        pltpu.VMEM((ROWS2, D), BF), pltpu.VMEM((NODES, D), F32),
                        pltpu.VMEM((D, D), BF), pltpu.VMEM((D, D), BF), pltpu.VMEM((2 * D, D), BF),
                        pltpu.SemaphoreType.DMA((5,))])
    return pl.pallas_call(
        edge_kernel,
        grid_spec=grid_spec,
        out_shape=jax.ShapeDtypeStruct((NODES, D), BF),
        compiler_params=pltpu.CompilerParams(vmem_limit_bytes=67043328, dimension_semantics=("arbitrary",)),
        cost_estimate=pl.CostEstimate(flops=flops, bytes_accessed=48 << 20, transcendentals=0),
        name="edges",
    )(src, dst, need, he, dst.reshape(steps, 1, ROWS2), mask.reshape(steps, 1, ROWS2), a0, vecs, proj, hm, table,
      w_second, w_edge_upd, w_mesh_upd)


def pad_features(x):
    ones = jnp.ones((x.shape[0], 1), BF)
    return jnp.concatenate([x.astype(BF), ones, jnp.zeros((x.shape[0], LANES - 1 - x.shape[1]), BF)], axis=1)


def pad_weight(w, bias):
    return jnp.concatenate([w, bias[None, :], jnp.zeros((LANES - 1 - w.shape[0], w.shape[1]), BF)], axis=0)


def solution(mesh):
    sharded = P(('batch', 'graph'))
    replicated = P()

    def local_step(grid_feat, mesh_feat, edge_feat, need_rows, edge_src, edge_dst, edge_mask,
                   w_grid_emb, w_mesh_emb, w_edge_emb, w_edge_upd, w_mesh_upd, w_grid_upd, w_second, mlp_vecs):
        xg = pad_features(grid_feat)
        table = lax.all_gather(xg, 'graph', axis=0, tiled=True)
        a0 = pad_weight(w_grid_emb, mlp_vecs[0, 0])
        a1 = pad_weight(w_mesh_emb, mlp_vecs[1, 0])
        a2 = pad_weight(w_edge_emb, mlp_vecs[2, 0])
        vecs = mlp_vecs.astype(F32).reshape(24, D)
        he, grid_out, hm, proj = run_embed(pad_features(edge_feat), a2, xg, a0, pad_features(mesh_feat), a1, vecs,
                                           w_second, w_edge_upd, w_grid_upd)
        mesh_out = run_edges(edge_src, edge_dst, need_rows, he, edge_mask, a0, vecs, proj, hm, table,
                             w_second, w_edge_upd, w_mesh_upd)
        return mesh_out, grid_out

    return jax.shard_map(local_step, mesh=mesh,
                         in_specs=(sharded,) * 7 + (replicated,) * 8,
                         out_specs=(sharded, sharded), check_vma=False)
```

```python
import jax
import jax.numpy as jnp
from jax import lax
from jax.experimental import pallas as pl
from jax.experimental.pallas import tpu as pltpu
from jax.sharding import PartitionSpec as P

LN_EPS = 1e-5
BF = jnp.bfloat16
F32 = jnp.float32
D = 1024
NODES = 512
EDGES = 8192
LANES = 128
BAND = 512
NB = D // LANES
SUB = 256
NC = 256
LN_ROWS = 32
ROWS = 512
CHUNK = 4096


def silu_half(h):
    return h + h * jnp.tanh(h)


def vec(vecs, mlp, k):
    return vecs[mlp, k:k + 1, :]


def layer_norm(x, gain, shift):
    mean = jnp.sum(x, axis=-1, keepdims=True) * (1.0 / D)
    c = x - mean
    var = jnp.sum(c * c, axis=-1, keepdims=True) * (1.0 / D)
    return c * lax.rsqrt(var + LN_EPS) * gain + shift


def wide(*pieces):
    return jnp.concatenate(pieces, axis=1)


def lhs(ref, r0):
    return wide(*[ref[j, r0:r0 + SUB, :] for j in range(NB)])


def rhs(ref, n):
    return wide(ref[2 * n], ref[2 * n + 1])


def put(ref, n, r0, y):
    ref[2 * n, r0:r0 + SUB, :] = y[:, :LANES]
    ref[2 * n + 1, r0:r0 + SUB, :] = y[:, LANES:]


def put_rows(ref, row, y):
    for j in range(NB):
        ref[j, row:row + LN_ROWS, :] = y[:, j * LANES:(j + 1) * LANES]


def get_rows(ref, row):
    return wide(*[ref[j, row:row + LN_ROWS, :] for j in range(NB)])


def cols(n):
    return slice(n * NC, (n + 1) * NC)


def dot(a, b):
    return jnp.dot(a, b, preferred_element_type=F32)


def second_layer(h, w, r, r0, bias):
    a = lhs(h, r0)
    for n in range(D // NC):
        r[r0:r0 + SUB, cols(n)] = dot(a, rhs(w, n)) + bias[:, cols(n)]


def norm_rows(r, r0, vecs, mlp, store):
    for q in range(r0, r0 + SUB, LN_ROWS):
        store(q, layer_norm(r[q:q + LN_ROWS, :], vec(vecs, mlp, 2), vec(vecs, mlp, 3)))


def column_copies(src, dst, sem):
    return [pltpu.make_async_copy(src.at[:, pl.ds(j * LANES, LANES)], dst.at[j], sem) for j in range(NB)]


def start(copies):
    for c in copies:
        c.start()


def wait(copies):
    for c in copies:
        c.wait()


def narrow_weights(dst, w, bias):
    k = w.shape[0]
    dst[...] = jnp.zeros_like(dst)
    dst[0:k, :] = 0.5 * w[...].astype(F32)
    dst[k:k + 1, :] = 0.5 * bias


def narrow_layer(xt, w, h, r0):
    x = xt[:, r0:r0 + SUB].T.astype(BF)
    for n in range(D // NC):
        put(h, n, r0, silu_half(dot(x, w[:, cols(n)].astype(BF))).astype(BF))


def grid_weights(dst, tmp, w, bias):
    k = w.shape[0]
    tmp[0:LANES, :] = jnp.zeros((LANES, D), F32)
    tmp[0:k, :] = 0.5 * w[...].astype(F32)
    tmp[k:k + 1, :] = 0.5 * bias
    for j in range(NB):
        dst[j] = tmp[0:LANES, j * LANES:(j + 1) * LANES].astype(BF)


def grid_layer(x, w, h, r0):
    for n in range(D // NC):
        put(h, n, r0, silu_half(dot(x, rhs(w, n))).astype(BF))


def full_layer(a, w, h, r0, bias):
    for n in range(D // NC):
        pre = dot(a, rhs(w, n)) + bias[:, cols(n)]
        put(h, n, r0, silu_half(0.5 * pre).astype(BF))


def embed_kernel(ef, mf, w_edge, w_mesh, vecs, wsec, wedge, he_out, hm_out, proj_out,
                 xt, a1, a2, h, r, b1, b2, w3, sems):
    i = pl.program_id(0)
    c1 = column_copies(wsec.at[1], b1, sems.at[0])
    c3 = column_copies(wedge.at[pl.ds(2 * D, D)], w3, sems.at[1])
    c2 = column_copies(wsec.at[2], b2, sems.at[2])
    blocks = range(0, ROWS, SUB)

    @pl.when(i == 0)
    def _():
        start(c1)
        start(c3)
        start(c2)
        narrow_weights(a1, w_mesh, vec(vecs, 1, 0))
        narrow_weights(a2, w_edge, vec(vecs, 2, 0))
        k = mf.shape[0]
        xt[...] = jnp.ones_like(xt)
        xt[0:k, :] = mf[...]
        for r0 in blocks:
            narrow_layer(xt, a1, h, r0)
        wait(c1)
        for r0 in blocks:
            second_layer(h, b1, r, r0, vec(vecs, 1, 1))
            norm_rows(r, r0, vecs, 1, lambda row, y: put_rows(hm_out, row, y.astype(BF)))
        wait(c3)
        for r0 in blocks:
            a = lhs(hm_out, r0)
            for n in range(D // NC):
                p = dot(a, rhs(w3, n)) + vec(vecs, 3, 0)[:, cols(n)]
                for t in range(2):
                    proj_out[pl.ds(r0 * 8 + 2 * n + t, SUB, stride=8), :] = p[:, t * LANES:(t + 1) * LANES]
        xt[...] = jnp.ones_like(xt)
        wait(c2)

    @pl.when(i > 0)
    def _():
        xt[0:ef.shape[0], :] = ef[...]
        for r0 in blocks:
            narrow_layer(xt, a2, h, r0)
        for r0 in blocks:
            second_layer(h, b2, r, r0, vec(vecs, 2, 1))
            norm_rows(r, r0, vecs, 2, lambda row, y: put_rows(he_out, row, y.astype(BF)))


def project_kernel(dst_s, he, proj, xg, w_grid, vecs, wedge, wsec, wgrid, pre_out, grid_out,
                   ga, gb, a0, emb, h, r, w1, b0, wg, b5, sems):
    i = pl.program_id(0)
    steps = EDGES // (2 * ROWS)
    c1 = column_copies(wedge.at[pl.ds(0, D)], w1, sems.at[0])
    c0 = column_copies(wsec.at[0], b0, sems.at[1])
    cg = column_copies(wgrid, wg, sems.at[2])
    c5 = column_copies(wsec.at[5], b5, sems.at[3])

    def fetch(buf, edge, row):
        d = dst_s[edge]
        buf[pl.ds(pl.multiple_of(row * 8, 8), 8), :] = proj[pl.ds(pl.multiple_of(d * 8, 8), 8), :]

    @pl.when(i == 0)
    def _():
        start(c1)
        start(c0)
        start(cg)
        start(c5)

        def fetch8(k, carry):
            for t in range(8):
                fetch(ga, k * 8 + t, k * 8 + t)
            return carry
        lax.fori_loop(0, ROWS // 8, fetch8, 0)
        wait(c1)

    @pl.when(i < steps)
    def _():
        base = i * (2 * ROWS)
        for half, (buf, other) in enumerate(((ga, gb), (gb, ga))):
            nxt = jnp.minimum(base + (half + 1) * ROWS, EDGES - ROWS)
            for e in range(ROWS):
                fetch(other, nxt + e, e)
            for r0 in range(0, ROWS, SUB):
                a = lhs(he, half * ROWS + r0)
                for n in range(D // NC):
                    p = dot(a, rhs(w1, n))
                    for t in range(2):
                        j = 2 * n + t
                        pre_out[half * ROWS + r0:half * ROWS + r0 + SUB, j * LANES:(j + 1) * LANES] = (
                            p[:, t * LANES:(t + 1) * LANES] + buf[pl.ds(r0 * 8 + j, SUB, stride=8), :])

    @pl.when(i == steps)
    def _():
        blocks = range(0, BAND, SUB)
        grid_weights(a0, r, w_grid, vec(vecs, 0, 0))
        wait(c0)
        wait(cg)
        wait(c5)
        for r0 in blocks:
            grid_layer(xg[r0:r0 + SUB, :], a0, h, r0)
        for r0 in blocks:
            second_layer(h, b0, r, r0, vec(vecs, 0, 1))
            norm_rows(r, r0, vecs, 0, lambda row, y: put_rows(emb, row, y.astype(BF)))
        for r0 in blocks:
            full_layer(lhs(emb, r0), wg, h, r0, vec(vecs, 5, 0))
        for r0 in blocks:
            second_layer(h, b5, r, r0, vec(vecs, 5, 1))

            def store(row, y):
                grid_out[row:row + LN_ROWS, :] = (get_rows(emb, row).astype(F32) + y).astype(BF)
            norm_rows(r, r0, vecs, 5, store)


def edge_kernel(src_s, need_s, par_s, he, pre, dst_v, mask_v, dst_p, mask_p, w_grid, vecs, hm, own, swapped,
                wsec, wedge, wmesh, mesh_out,
                ftab, stage, xg, a0, h, r, hg, newx, newy, acc, b0, b3, w2, wm, sems):
    i = pl.program_id(0)
    steps = EDGES // ROWS
    c0 = column_copies(wsec.at[0], b0, sems.at[2])
    c2 = column_copies(wedge.at[pl.ds(D, D)], w2, sems.at[3])
    c3 = column_copies(wsec.at[3], b3, sems.at[4])
    cm = column_copies(wmesh, wm, sems.at[5])
    c4 = column_copies(wsec.at[4], b0, sems.at[6])
    per = own.shape[0] // CHUNK

    def stage_copy(c):
        src = own if c < per else swapped
        return pltpu.make_async_copy(src.at[pl.ds((c % per) * CHUNK, CHUNK)], stage.at[c % 2], sems.at[c % 2])

    def fetch_row(edge, row):
        s = src_s[edge]
        g = lax.shift_right_logical(s, 6) * BAND + need_s[s]
        xg[pl.ds(row, 1), :] = ftab[pl.ds(g, 1), :]

    @pl.when(i == 0)
    def _():
        stage_copy(0).start()
        stage_copy(1).start()
        start(c0)
        start(c2)
        start(c3)
        parity = par_s[0]
        grid_weights(a0, r, w_grid, vec(vecs, 0, 0))
        acc[...] = jnp.zeros_like(acc)
        newy[...] = jnp.zeros_like(newy)
        for c in range(2 * per):
            stage_copy(c).wait()
            owner = parity if c < per else 1 - parity

            def part(k, carry):
                band = 2 * ((c % per) * (CHUNK // BAND) + k) + owner
                for half in range(2):
                    piece = stage[c % 2, pl.ds(pl.multiple_of(k * BAND + half * 256, 256), 256), :]
                    ftab[pl.ds(pl.multiple_of(band * BAND + half * 256, 256), 256), :] = piece.astype(F32)
                return carry
            lax.fori_loop(0, CHUNK // BAND, part, 0)
            if c + 2 < 2 * per:
                stage_copy(c + 2).start()
        start(cm)

        def fetch8(k, carry):
            for t in range(8):
                fetch_row(k * 8 + t, k * 8 + t)
            return carry
        lax.fori_loop(0, ROWS // 8, fetch8, 0)
        wait(c0)
        wait(c2)
        wait(c3)

    def aggregate(dst_ref, mask_ref, r0, new):
        node = lax.broadcasted_iota(jnp.int32, (NODES, SUB), 0)
        dst = jnp.where(mask_ref[0, :, r0:r0 + SUB] > 0, dst_ref[0, :, r0:r0 + SUB], -1)
        inc = jnp.where(node == dst, 1.0, 0.0).astype(BF)
        for n in range(D // NC):
            acc[:, cols(n)] += dot(inc, rhs(new, n))

    def update(r0, new):
        second_layer(h, b3, r, r0, vec(vecs, 3, 1))

        def store(row, y):
            put_rows(new, row - r0, (get_rows(he, row).astype(F32) + y).astype(BF))
        norm_rows(r, r0, vecs, 3, store)

    blocks = range(0, ROWS, SUB)
    for r0 in blocks:
        grid_layer(xg[r0:r0 + SUB, :].astype(BF), a0, h, r0)
    after = jnp.minimum(i + 1, steps - 1) * ROWS
    for e in range(ROWS):
        fetch_row(after + e, e)
    for r0 in blocks:
        second_layer(h, b0, r, r0, vec(vecs, 0, 1))
        norm_rows(r, r0, vecs, 0, lambda row, y: put_rows(hg, row, y.astype(BF)))
    for r0 in blocks:
        a = lhs(hg, r0)
        for n in range(D // NC):
            x = dot(a, rhs(w2, n)) + pre[r0:r0 + SUB, cols(n)]
            put(h, n, r0, silu_half(0.5 * x).astype(BF))
    update(0, newx)
    aggregate(dst_p, mask_p, SUB, newy)
    update(SUB, newy)
    aggregate(dst_v, mask_v, 0, newx)

    @pl.when(i == steps - 1)
    def _():
        start(c4)
        aggregate(dst_v, mask_v, SUB, newy)
        for j in range(NB):
            hg[j] = acc[:, j * LANES:(j + 1) * LANES].astype(BF)
        wait(cm)
        for r0 in range(0, NODES, SUB):
            full_layer(wide(lhs(hm, r0), lhs(hg, r0)), wm, h, r0, vec(vecs, 4, 0))
        wait(c4)
        for r0 in range(0, NODES, SUB):
            second_layer(h, b0, r, r0, vec(vecs, 4, 1))

            def store(row, y):
                mesh_out[row:row + LN_ROWS, :] = (get_rows(hm, row).astype(F32) + y).astype(BF)
            norm_rows(r, r0, vecs, 4, store)


def fixed(shape):
    return pl.BlockSpec(shape, lambda i, *_: (0,) * len(shape), pipeline_mode=pl.Buffered(1))


ANY = pl.BlockSpec(memory_space=pl.ANY)
SQUARE = pltpu.VMEM((NB, D, LANES), BF)
HIDDEN = pltpu.VMEM((NB, ROWS, LANES), BF)
RESULT = pltpu.VMEM((ROWS, D), F32)
VECS = (6, 4, D)


def params(limit):
    return pltpu.CompilerParams(vmem_limit_bytes=limit, dimension_semantics=("arbitrary",))


def cost(macs, size):
    return pl.CostEstimate(flops=2 * macs, bytes_accessed=size, transcendentals=0)


def run_embed(edge_t, mesh_t, w_edge_emb, w_mesh_emb, vecs, w_second, w_edge_upd):
    steps = EDGES // ROWS
    before = lambda i: jnp.maximum(i - 1, 0)
    return pl.pallas_call(
        embed_kernel,
        grid=(steps + 1,),
        in_specs=[pl.BlockSpec((edge_t.shape[0], ROWS), lambda i: (0, before(i))), fixed(mesh_t.shape),
                  fixed(w_edge_emb.shape), fixed(w_mesh_emb.shape), fixed(VECS), ANY, ANY],
        out_specs=[pl.BlockSpec((NB, ROWS, LANES), lambda i: (0, before(i), 0)),
                   fixed((NB, NODES, LANES)), fixed((NODES * 8, LANES))],
        out_shape=[jax.ShapeDtypeStruct((NB, EDGES, LANES), BF), jax.ShapeDtypeStruct((NB, NODES, LANES), BF),
                   jax.ShapeDtypeStruct((NODES * 8, LANES), F32)],
        scratch_shapes=[pltpu.VMEM((8, ROWS), F32), pltpu.VMEM((8, D), F32), pltpu.VMEM((8, D), F32), HIDDEN, RESULT,
                        SQUARE, SQUARE, SQUARE, pltpu.SemaphoreType.DMA((3,))],
        compiler_params=params(40 << 20),
        cost_estimate=cost(EDGES * D * (D + 256) + NODES * D * (2 * D + 256), 26 << 20),
        name="embed",
    )(edge_t, mesh_t, w_edge_emb, w_mesh_emb, vecs, w_second, w_edge_upd)


def run_project(dst, he, proj, xg, w_grid_emb, vecs, w_edge_upd, w_second, w_grid_upd):
    steps = EDGES // (2 * ROWS)
    block = lambda i: jnp.minimum(i, steps - 1)
    grid_spec = pltpu.PrefetchScalarGridSpec(
        num_scalar_prefetch=1,
        grid=(steps + 1,),
        in_specs=[pl.BlockSpec((NB, 2 * ROWS, LANES), lambda i, *_: (0, block(i), 0)), fixed((NODES * 8, LANES)),
                  fixed((BAND, LANES)), fixed(w_grid_emb.shape), fixed(VECS), ANY, ANY, ANY],
        out_specs=[pl.BlockSpec((2 * ROWS, D), lambda i, *_: (block(i), 0)), fixed((BAND, D))],
        scratch_shapes=[pltpu.VMEM((ROWS * 8, LANES), F32), pltpu.VMEM((ROWS * 8, LANES), F32),
                        pltpu.VMEM((NB, LANES, LANES), BF), HIDDEN, HIDDEN, RESULT,
                        SQUARE, SQUARE, SQUARE, SQUARE, pltpu.SemaphoreType.DMA((4,))])
    return pl.pallas_call(
        project_kernel,
        grid_spec=grid_spec,
        out_shape=[jax.ShapeDtypeStruct((EDGES, D), F32), jax.ShapeDtypeStruct((BAND, D), BF)],
        compiler_params=params(48 << 20),
        cost_estimate=cost(EDGES * D * D + BAND * D * (3 * D + 256), 58 << 20),
        name="project",
    )(dst, he, proj, xg, w_grid_emb, vecs, w_edge_upd, w_second, w_grid_upd)


def run_edges(src, need, parity, he, pre, dst, mask, w_grid_emb, vecs, hm, own, swapped, w_second, w_edge_upd, w_mesh_upd):
    steps = EDGES // ROWS
    here = pl.BlockSpec((1, 1, ROWS), lambda i, *_: (i, 0, 0))
    before = pl.BlockSpec((1, 1, ROWS), lambda i, *_: (jnp.maximum(i - 1, 0), 0, 0))
    grid_spec = pltpu.PrefetchScalarGridSpec(
        num_scalar_prefetch=3,
        grid=(steps,),
        in_specs=[pl.BlockSpec((NB, ROWS, LANES), lambda i, *_: (0, i, 0)), pl.BlockSpec((ROWS, D), lambda i, *_: (i, 0)),
                  here, here, before, before, fixed(w_grid_emb.shape), fixed(VECS), fixed((NB, NODES, LANES)),
                  ANY, ANY, ANY, ANY, ANY],
        out_specs=fixed((NODES, D)),
        scratch_shapes=[pltpu.VMEM((2 * own.shape[0], LANES), F32), pltpu.VMEM((2, CHUNK, LANES), BF),
                        pltpu.VMEM((ROWS, LANES), F32), pltpu.VMEM((NB, LANES, LANES), BF), HIDDEN, RESULT, HIDDEN,
                        pltpu.VMEM((NB, SUB, LANES), BF), pltpu.VMEM((NB, SUB, LANES), BF), pltpu.VMEM((NODES, D), F32),
                        SQUARE, SQUARE, SQUARE, pltpu.VMEM((NB, 2 * D, LANES), BF),
                        pltpu.SemaphoreType.DMA((7,))])
    dst = dst.reshape(steps, 1, ROWS)
    mask = mask.reshape(steps, 1, ROWS)
    return pl.pallas_call(
        edge_kernel,
        grid_spec=grid_spec,
        out_shape=jax.ShapeDtypeStruct((NODES, D), BF),
        compiler_params=params(67043328),
        cost_estimate=cost(EDGES * D * (3 * D + 256 + NODES) + NODES * 3 * D * D, 80 << 20),
        name="edges",
    )(src, need, parity, he, pre, dst, mask, dst, mask, w_grid_emb, vecs, hm, own, swapped, w_second, w_edge_upd, w_mesh_upd)


def pad_features(x):
    ones = jnp.ones((x.shape[0], 1), BF)
    return jnp.concatenate([x.astype(BF), ones, jnp.zeros((x.shape[0], LANES - 1 - x.shape[1]), BF)], axis=1)


def gather_own(xg, size):
    return lax.all_gather(xg, 'graph', axis=0, tiled=True,
                          axis_index_groups=[list(range(0, size, 2)), list(range(1, size, 2))])


def swap_halves(own, size):
    swapped = lax.ppermute(own, 'graph', [(k, k ^ 1) for k in range(size)])
    return swapped, lax.rem(lax.axis_index('graph'), 2).astype(jnp.int32).reshape(1)


def solution(mesh):
    size = mesh.shape['graph']
    sharded = P(('batch', 'graph'))
    replicated = P()

    def local_step(grid_feat, mesh_feat, edge_feat, need_rows, edge_src, edge_dst, edge_mask,
                   w_grid_emb, w_mesh_emb, w_edge_emb, w_edge_upd, w_mesh_upd, w_grid_upd, w_second, mlp_vecs):
        xg = pad_features(grid_feat)
        own = gather_own(xg, size)
        vecs = mlp_vecs.astype(F32)
        he, hm, proj = run_embed(edge_feat.T, mesh_feat.T, w_edge_emb, w_mesh_emb, vecs, w_second, w_edge_upd)
        own, he = lax.optimization_barrier((own, he))
        swapped, parity = swap_halves(own, size)
        pre, grid_out = run_project(edge_dst, he, proj, xg, w_grid_emb, vecs, w_edge_upd, w_second, w_grid_upd)
        mesh_out = run_edges(edge_src, need_rows, parity, he, pre, edge_dst, edge_mask, w_grid_emb, vecs, hm, own, swapped,
                             w_second, w_edge_upd, w_mesh_upd)
        return mesh_out, grid_out

    return jax.shard_map(local_step, mesh=mesh,
                         in_specs=(sharded,) * 7 + (replicated,) * 8,
                         out_specs=(sharded, sharded), check_vma=False)
```

```python
import jax
import jax.numpy as jnp
from jax import lax
from jax.experimental import pallas as pl
from jax.experimental.pallas import tpu as pltpu
from jax.sharding import PartitionSpec as P

LN_EPS = 1e-5
BF = jnp.bfloat16
F32 = jnp.float32
D = 1024
NODES = 512
EDGES = 8192
LANES = 128
BAND = 512
NB = D // LANES
SUB = 256
NC = 256
LN_ROWS = 32
ROWS = 512
ROWS_E = 2048
PICK = 1024


def silu_half(h):
    return h + h * jnp.tanh(h)


def vec(vecs, mlp, k):
    return vecs[mlp, k:k + 1, :]


def layer_norm(x, gain, shift):
    mean = jnp.sum(x, axis=-1, keepdims=True) * (1.0 / D)
    c = x - mean
    var = jnp.sum(c * c, axis=-1, keepdims=True) * (1.0 / D)
    return c * lax.rsqrt(var + LN_EPS) * gain + shift


def wide(*pieces):
    return jnp.concatenate(pieces, axis=1)


def lhs(ref, r0):
    return wide(*[ref[j, r0:r0 + SUB, :] for j in range(NB)])


def rhs(ref, n):
    return wide(ref[2 * n], ref[2 * n + 1])


def put(ref, n, r0, y):
    ref[2 * n, r0:r0 + SUB, :] = y[:, :LANES]
    ref[2 * n + 1, r0:r0 + SUB, :] = y[:, LANES:]


def put_rows(ref, row, y):
    for j in range(NB):
        ref[j, row:row + LN_ROWS, :] = y[:, j * LANES:(j + 1) * LANES]


def get_rows(ref, row):
    return wide(*[ref[j, row:row + LN_ROWS, :] for j in range(NB)])


def cols(n):
    return slice(n * NC, (n + 1) * NC)


def dot(a, b):
    return jnp.dot(a, b, preferred_element_type=F32)


def second_layer(h, w, r, r0, bias):
    a = lhs(h, r0)
    for n in range(D // NC):
        r[r0:r0 + SUB, cols(n)] = dot(a, rhs(w, n)) + bias[:, cols(n)]


def norm_rows(r, r0, vecs, mlp, store):
    for q in range(r0, r0 + SUB, LN_ROWS):
        store(q, layer_norm(r[q:q + LN_ROWS, :], vec(vecs, mlp, 2), vec(vecs, mlp, 3)))


def column_copies(src, dst, sem):
    return [pltpu.make_async_copy(src.at[:, pl.ds(j * LANES, LANES)], dst.at[j], sem) for j in range(NB)]


def start(copies):
    for c in copies:
        c.start()


def wait(copies):
    for c in copies:
        c.wait()


def narrow_weights(dst, w, bias):
    k = w.shape[0]
    dst[...] = jnp.zeros_like(dst)
    dst[0:k, :] = 0.5 * w[...].astype(F32)
    dst[k:k + 1, :] = 0.5 * bias


def narrow_layer(xt, w, h, r0):
    x = xt[:, r0:r0 + SUB].T.astype(BF)
    for n in range(D // NC):
        put(h, n, r0, silu_half(dot(x, w[:, cols(n)].astype(BF))).astype(BF))


def grid_weights(dst, tmp, w, bias):
    k = w.shape[0]
    tmp[0:LANES, :] = jnp.zeros((LANES, D), F32)
    tmp[0:k, :] = 0.5 * w[...].astype(F32)
    tmp[k:k + 1, :] = 0.5 * bias
    for j in range(NB):
        dst[j] = tmp[0:LANES, j * LANES:(j + 1) * LANES].astype(BF)


def grid_layer(x, w, h, r0):
    for n in range(D // NC):
        put(h, n, r0, silu_half(dot(x, rhs(w, n))).astype(BF))


def full_layer(a, w, h, r0, bias):
    for n in range(D // NC):
        pre = dot(a, rhs(w, n)) + bias[:, cols(n)]
        put(h, n, r0, silu_half(0.5 * pre).astype(BF))


def node_kernel(mf, xg, w_mesh, w_grid, vecs, wsec, wedge, wgrid, hm_out, proj_out, grid_out,
                xt, a1, a0, emb, h, r, b1, w3, b0, wg, b5, sems):
    copies = [column_copies(wsec.at[1], b1, sems.at[0]), column_copies(wedge.at[pl.ds(2 * D, D)], w3, sems.at[1]),
              column_copies(wsec.at[0], b0, sems.at[2]), column_copies(wgrid, wg, sems.at[3]),
              column_copies(wsec.at[5], b5, sems.at[4])]
    for c in copies:
        start(c)
    blocks = range(0, NODES, SUB)
    narrow_weights(a1, w_mesh, vec(vecs, 1, 0))
    grid_weights(a0, r, w_grid, vec(vecs, 0, 0))
    xt[...] = jnp.ones_like(xt)
    xt[0:mf.shape[0], :] = mf[...]
    for r0 in blocks:
        narrow_layer(xt, a1, h, r0)
    wait(copies[0])
    for r0 in blocks:
        second_layer(h, b1, r, r0, vec(vecs, 1, 1))
        norm_rows(r, r0, vecs, 1, lambda row, y: put_rows(hm_out, row, y.astype(BF)))
    wait(copies[1])
    for r0 in blocks:
        a = lhs(hm_out, r0)
        for n in range(D // NC):
            p = dot(a, rhs(w3, n)) + vec(vecs, 3, 0)[:, cols(n)]
            for t in range(2):
                proj_out[pl.ds(r0 * 8 + 2 * n + t, SUB, stride=8), :] = p[:, t * LANES:(t + 1) * LANES]
    for r0 in blocks:
        grid_layer(xg[r0:r0 + SUB, :], a0, h, r0)
    wait(copies[2])
    for r0 in blocks:
        second_layer(h, b0, r, r0, vec(vecs, 0, 1))
        norm_rows(r, r0, vecs, 0, lambda row, y: put_rows(emb, row, y.astype(BF)))
    wait(copies[3])
    for r0 in blocks:
        full_layer(lhs(emb, r0), wg, h, r0, vec(vecs, 5, 0))
    wait(copies[4])
    for r0 in blocks:
        second_layer(h, b5, r, r0, vec(vecs, 5, 1))

        def store(row, y):
            grid_out[row:row + LN_ROWS, :] = (get_rows(emb, row).astype(F32) + y).astype(BF)
        norm_rows(r, r0, vecs, 5, store)


def select_kernel(req, xg, out):
    xt = xg[...].T
    for k in range(EDGES // PICK):
        ids = req[:, k * PICK:(k + 1) * PICK]
        row = lax.broadcasted_iota(jnp.int32, (BAND, PICK), 0)
        hot = jnp.where(row == ids, 1.0, 0.0).astype(BF)
        out[k * PICK:(k + 1) * PICK, :] = dot(xt, hot).T.astype(BF)


def embed_kernel(ef, w_edge, vecs, wsec, he_out, xt, a2, h, r, b2, sems):
    c2 = column_copies(wsec.at[2], b2, sems.at[0])
    blocks = range(0, ROWS_E, SUB)

    @pl.when(pl.program_id(0) == 0)
    def _():
        start(c2)
        narrow_weights(a2, w_edge, vec(vecs, 2, 0))
        xt[...] = jnp.ones_like(xt)
        wait(c2)
    xt[0:ef.shape[0], :] = ef[...]
    narrow_layer(xt, a2, h, 0)
    for r0 in blocks:
        if r0 + SUB < ROWS_E:
            narrow_layer(xt, a2, h, r0 + SUB)
        second_layer(h, b2, r, r0, vec(vecs, 2, 1))
        norm_rows(r, r0, vecs, 2, lambda row, y: put_rows(he_out, row, y.astype(BF)))


def edge_kernel(src_s, dst_s, he, dst_v, mask_v, dst_p, mask_p, w_grid, vecs, hm, proj, table, wsec, wedge, wmesh, mesh_out,
                ftab, xg, gm, a0, h, r, ry, hg, newx, newy, hey, acc, b0, b3, w12, wm, b4, sems):
    i = pl.program_id(0)
    steps = EDGES // ROWS
    c0 = column_copies(wsec.at[0], b0, sems.at[0])
    c1 = column_copies(wedge.at[pl.ds(0, 2 * D)], w12, sems.at[1])
    c3 = column_copies(wsec.at[3], b3, sems.at[2])
    cm = column_copies(wmesh, wm, sems.at[3])
    c4 = column_copies(wsec.at[4], b4, sems.at[4])

    def fetch_row(edge, row):
        xg[pl.ds(row, 1), :] = ftab[pl.ds(src_s[edge], 1), :]

    @pl.when(i == 0)
    def _():
        for c in (c0, c1, c3, cm, c4):
            start(c)
        grid_weights(a0, r, w_grid, vec(vecs, 0, 0))
        acc[...] = jnp.zeros_like(acc)
        ry[...] = jnp.zeros_like(ry)
        hey[...] = jnp.zeros_like(hey)

        def widen(k, carry):
            rows = pl.ds(pl.multiple_of(k * 256, 256), 256)
            ftab[rows, :] = table[rows, :].astype(F32)
            return carry
        lax.fori_loop(0, EDGES // 256, widen, 0)

        def fetch8(k, carry):
            for t in range(8):
                fetch_row(k * 8 + t, k * 8 + t)
            return carry
        lax.fori_loop(0, ROWS // 8, fetch8, 0)
        for c in (c0, c1, c3):
            wait(c)

    def aggregate(dst, mask, new):
        node = lax.broadcasted_iota(jnp.int32, (NODES, SUB), 0)
        inc = jnp.where(node == jnp.where(mask > 0, dst, -1), 1.0, 0.0).astype(BF)
        for n in range(D // NC):
            acc[:, cols(n)] += dot(inc, rhs(new, n))

    def store_y(row, y):
        put_rows(newy, row, (get_rows(hey, row).astype(F32) + y).astype(BF))

    blocks = range(0, ROWS, SUB)
    for r0 in blocks:
        grid_layer(xg[r0:r0 + SUB, :].astype(BF), a0, h, r0)
    base = i * ROWS
    after = jnp.minimum(i + 1, steps - 1) * ROWS
    for e in range(ROWS):
        d = dst_s[base + e]
        gm[e * 8:(e + 1) * 8, :] = proj[pl.ds(pl.multiple_of(d * 8, 8), 8), :]
        fetch_row(after + e, e)
    norm_rows(ry, 0, vecs, 3, store_y)
    for r0 in blocks:
        second_layer(h, b0, r, r0, vec(vecs, 0, 1))
        norm_rows(r, r0, vecs, 0, lambda row, y: put_rows(hg, row, y.astype(BF)))
    for r0 in blocks:
        a = wide(lhs(he, r0), lhs(hg, r0))
        for n in range(D // NC):
            x = dot(a, rhs(w12, n))
            x = x + wide(*[gm[pl.ds(r0 * 8 + 2 * n + t, SUB, stride=8), :] for t in range(2)])
            put(h, n, r0, silu_half(0.5 * x).astype(BF))
    second_layer(h, b3, r, 0, vec(vecs, 3, 1))

    def store_x(row, y):
        put_rows(newx, row, (get_rows(he, row).astype(F32) + y).astype(BF))
    norm_rows(r, 0, vecs, 3, store_x)
    aggregate(dst_p[0, :, SUB:], mask_p[0, :, SUB:] * jnp.minimum(i, 1), newy)
    a = lhs(h, SUB)
    for n in range(D // NC):
        ry[:, cols(n)] = dot(a, rhs(b3, n)) + vec(vecs, 3, 1)[:, cols(n)]
    for j in range(NB):
        hey[j] = he[j, SUB:, :]
    aggregate(dst_v[0, :, :SUB], mask_v[0, :, :SUB], newx)

    @pl.when(i == steps - 1)
    def _():
        norm_rows(ry, 0, vecs, 3, store_y)
        wait(cm)
        wait(c4)
        aggregate(dst_v[0, :, SUB:], mask_v[0, :, SUB:], newy)
        for j in range(NB):
            hg[j] = acc[:, j * LANES:(j + 1) * LANES].astype(BF)
        for r0 in range(0, NODES, SUB):
            full_layer(wide(lhs(hm, r0), lhs(hg, r0)), wm, h, r0, vec(vecs, 4, 0))
        for r0 in range(0, NODES, SUB):
            second_layer(h, b4, r, r0, vec(vecs, 4, 1))

            def store(row, y):
                mesh_out[row:row + LN_ROWS, :] = (get_rows(hm, row).astype(F32) + y).astype(BF)
            norm_rows(r, r0, vecs, 4, store)


def fixed(shape):
    return pl.BlockSpec(shape, lambda i, *_: (0,) * len(shape), pipeline_mode=pl.Buffered(1))


FAR = pl.BlockSpec(memory_space=pltpu.HBM)
SQUARE = pltpu.VMEM((NB, D, LANES), BF)
HIDDEN = pltpu.VMEM((NB, ROWS, LANES), BF)
HALF = pltpu.VMEM((NB, SUB, LANES), BF)
RESULT = pltpu.VMEM((ROWS, D), F32)
VECS = (6, 4, D)
PARAMS = pltpu.CompilerParams(vmem_limit_bytes=67043328, dimension_semantics=("arbitrary",))


def cost(macs, size):
    return pl.CostEstimate(flops=2 * macs, bytes_accessed=size, transcendentals=0)


def run_nodes(mesh_t, xg, w_mesh_emb, w_grid_emb, vecs, w_second, w_edge_upd, w_grid_upd):
    return pl.pallas_call(
        node_kernel,
        grid=(1,),
        in_specs=[fixed(mesh_t.shape), fixed((BAND, LANES)), fixed(w_mesh_emb.shape), fixed(w_grid_emb.shape), fixed(VECS),
                  FAR, FAR, FAR],
        out_specs=[fixed((NB, NODES, LANES)), fixed((NODES * 8, LANES)), fixed((BAND, D))],
        out_shape=[jax.ShapeDtypeStruct((NB, NODES, LANES), BF), jax.ShapeDtypeStruct((NODES * 8, LANES), F32),
                   jax.ShapeDtypeStruct((BAND, D), BF)],
        scratch_shapes=[pltpu.VMEM((8, NODES), F32), pltpu.VMEM((8, D), F32), pltpu.VMEM((NB, LANES, LANES), BF), HIDDEN,
                        HIDDEN, RESULT, SQUARE, SQUARE, SQUARE, SQUARE, SQUARE, pltpu.SemaphoreType.DMA((5,))],
        compiler_params=PARAMS,
        cost_estimate=cost(NODES * D * (5 * D + 512), 16 << 20),
        name="nodes",
    )(mesh_t, xg, w_mesh_emb, w_grid_emb, vecs, w_second, w_edge_upd, w_grid_upd)


def run_select(req, xg):
    return pl.pallas_call(
        select_kernel,
        grid=(1,),
        in_specs=[fixed((1, EDGES)), fixed((BAND, LANES))],
        out_specs=fixed((EDGES, LANES)),
        out_shape=jax.ShapeDtypeStruct((EDGES, LANES), BF),
        compiler_params=PARAMS,
        cost_estimate=cost(EDGES * BAND * LANES, 3 << 20),
        name="select",
    )(req, xg)


def run_embed(edge_t, w_edge_emb, vecs, w_second):
    return pl.pallas_call(
        embed_kernel,
        grid=(EDGES // ROWS_E,),
        in_specs=[pl.BlockSpec((edge_t.shape[0], ROWS_E), lambda i: (0, i)), fixed(w_edge_emb.shape), fixed(VECS), FAR],
        out_specs=pl.BlockSpec((NB, ROWS_E, LANES), lambda i: (0, i, 0)),
        out_shape=jax.ShapeDtypeStruct((NB, EDGES, LANES), BF),
        scratch_shapes=[pltpu.VMEM((8, ROWS_E), F32), pltpu.VMEM((8, D), F32), pltpu.VMEM((NB, ROWS_E, LANES), BF),
                        pltpu.VMEM((ROWS_E, D), F32), SQUARE, pltpu.SemaphoreType.DMA((1,))],
        compiler_params=PARAMS,
        cost_estimate=cost(EDGES * D * (D + 256), 18 << 20),
        name="embed",
    )(edge_t, w_edge_emb, vecs, w_second)


def run_edges(src, dst, he, mask, w_grid_emb, vecs, hm, proj, table, w_second, w_edge_upd, w_mesh_upd):
    steps = EDGES // ROWS
    here = pl.BlockSpec((1, 1, ROWS), lambda i, *_: (i, 0, 0))
    before = pl.BlockSpec((1, 1, ROWS), lambda i, *_: (jnp.maximum(i - 1, 0), 0, 0))
    grid_spec = pltpu.PrefetchScalarGridSpec(
        num_scalar_prefetch=2,
        grid=(steps,),
        in_specs=[pl.BlockSpec((NB, ROWS, LANES), lambda i, *_: (0, i, 0)), here, here, before, before,
                  fixed(w_grid_emb.shape), fixed(VECS), fixed((NB, NODES, LANES)), fixed((NODES * 8, LANES)),
                  fixed((EDGES, LANES)), FAR, FAR, FAR],
        out_specs=fixed((NODES, D)),
        scratch_shapes=[pltpu.VMEM((EDGES, LANES), F32), pltpu.VMEM((ROWS, LANES), F32), pltpu.VMEM((ROWS * 8, LANES), F32),
                        pltpu.VMEM((NB, LANES, LANES), BF), HIDDEN, RESULT, pltpu.VMEM((SUB, D), F32), HIDDEN,
                        HALF, HALF, HALF, pltpu.VMEM((NODES, D), F32),
                        SQUARE, SQUARE, pltpu.VMEM((NB, 2 * D, LANES), BF), pltpu.VMEM((NB, 2 * D, LANES), BF), SQUARE,
                        pltpu.SemaphoreType.DMA((5,))])
    dst3 = dst.reshape(steps, 1, ROWS)
    mask3 = mask.reshape(steps, 1, ROWS)
    return pl.pallas_call(
        edge_kernel,
        grid_spec=grid_spec,
        out_shape=jax.ShapeDtypeStruct((NODES, D), BF),
        compiler_params=PARAMS,
        cost_estimate=cost(EDGES * D * (4 * D + 256 + NODES) + NODES * 3 * D * D, 40 << 20),
        name="edges",
    )(src, dst, he, dst3, mask3, dst3, mask3, w_grid_emb, vecs, hm, proj, table, w_second, w_edge_upd, w_mesh_upd)


def pad_features(x):
    ones = jnp.ones((x.shape[0], 1), BF)
    return jnp.concatenate([x.astype(BF), ones, jnp.zeros((x.shape[0], LANES - 1 - x.shape[1]), BF)], axis=1)


def exchange(x):
    return lax.all_to_all(x, 'graph', 0, 0, tiled=True)


def solution(mesh):
    size = mesh.shape['graph']
    sharded = P(('batch', 'graph'))
    replicated = P()

    def local_step(grid_feat, mesh_feat, edge_feat, need_rows, edge_src, edge_dst, edge_mask,
                   w_grid_emb, w_mesh_emb, w_edge_emb, w_edge_upd, w_mesh_upd, w_grid_upd, w_second, mlp_vecs):
        slots = need_rows.shape[0] // size
        wanted = exchange(need_rows.reshape(size, slots))
        xg = pad_features(grid_feat)
        vecs = mlp_vecs.astype(F32)
        hm, proj, grid_out = run_nodes(mesh_feat.T, xg, w_mesh_emb, w_grid_emb, vecs, w_second, w_edge_upd, w_grid_upd)
        wanted, hm = lax.optimization_barrier((wanted, hm))
        rows = run_select(wanted.reshape(1, size * slots), xg)
        rows, vecs = lax.optimization_barrier((rows, vecs))
        table = exchange(rows.reshape(size, slots, LANES)).reshape(size * slots, LANES)
        he = run_embed(edge_feat.T, w_edge_emb, vecs, w_second)
        mesh_out = run_edges(edge_src, edge_dst, he, edge_mask, w_grid_emb, vecs, hm, proj, table,
                             w_second, w_edge_upd, w_mesh_upd)
        return mesh_out, grid_out

    return jax.shard_map(local_step, mesh=mesh,
                         in_specs=(sharded,) * 7 + (replicated,) * 8,
                         out_specs=(sharded, sharded), check_vma=False)
```
